256 devices in a mesh: leaf: 8 (over z_hi, core), seq: 32 (over x, z_lo, y).
Axes of the slice: x: 4, y: 4, z: 8 (z_hi: 4, z_lo: 2; z = z_hi * 2 + z_lo), core: 2. Of those that a mesh axis runs over, the one named last changes fastest.
Arguments:
- queries: bfloat16 [8, 8192, 4096], P('leaf', 'seq'), may hold values from -40 to 40
- branch_key_rows: bfloat16 [8, 8192, 512], P('leaf', 'seq'), may hold values from -6 to 6
- branch_value_rows: bfloat16 [8, 8192, 512], P('leaf', 'seq'), may hold values from -6 to 6
- grad_output: bfloat16 [8, 8192, 4096], P('leaf', 'seq'), may hold values from -6 to 6
- trunk_keys: bfloat16 [8, 256, 512], P('leaf', 'seq'), may hold values from -6 to 6
- trunk_token_values: bfloat16 [8, 256, 512], P('leaf', 'seq'), may hold values from -6 to 6
- lengths: int32 [8, 128], P(None, 'seq'), may hold values from 0 to 64, as said below
- parents: int32 [8, 128], P(None, 'seq'), may hold values from 1 to 255
Outputs:
- grad_queries: float32 [8, 8192, 4096], P('leaf', 'seq')
- grad_branch_keys: float32 [8, 8192, 512], P('leaf', 'seq')
- grad_branch_values: float32 [8, 8192, 512], P('leaf', 'seq')
- grad_trunk_keys: float32 [8, 256, 512], P('leaf', 'seq')
- grad_trunk_values: float32 [8, 256, 512], P('leaf', 'seq')
The draws below stay inside these ranges and needn't reach their ends.
Inputs may be any that keep to these rules, and one draw needn't show every extreme that they name: `lengths`: 0 means that the slot holds no branch.
All inputs are finite; a program needn't handle non-finite values.
Results may differ from the reference program's by a relative error of at most 0.0052.
Values may be sent and summed in bfloat16 or wider, within the bound.
No kernel may reach another device: no remote copies, remote signals or barrier semaphores. Data moves between devices by JAX's collectives and lax.ppermute only.
A program may use at most 64 MiB of HBM per device.

```python
import math
import jax
import jax.numpy as jnp
from jax import lax

QUERY_HEADS = 32
KEY_VALUE_HEADS = 4
HEAD_SIZE = 128
TRUNK_TOKENS = 256
TILE_ROWS = 64
TILES_DEV = 4
ROLLOUT_TREES = 8
BRANCH_SLOTS = 128


def trunk_base(key):
    drawn_values = jnp.clip(jax.random.normal(jax.random.fold_in(key, 11), (ROLLOUT_TREES, TRUNK_TOKENS, KEY_VALUE_HEADS * HEAD_SIZE), jnp.float32), -6.0, 6.0)
    return drawn_values


def draw_trunk_keys(key, part):
    return trunk_base(key).astype(jnp.bfloat16)


def draw_queries(key, part):
    drawn_values = jnp.clip(jax.random.normal(jax.random.fold_in(key, 21), (ROLLOUT_TREES, BRANCH_SLOTS * TILE_ROWS, QUERY_HEADS * HEAD_SIZE), jnp.float32), -6.0, 6.0)
    return drawn_values.astype(jnp.bfloat16)


def draw_lengths(key, part):
    half_trees = ROLLOUT_TREES // 2
    tree_ids = jnp.arange(ROLLOUT_TREES)[:, None]
    heavy_side = jax.random.randint(jax.random.fold_in(key, 37), (half_trees,), 0, 2)
    side_of_tree = jnp.concatenate([heavy_side, 1 - heavy_side])[:, None]
    heavy_level = jax.random.randint(jax.random.fold_in(key, 31), (ROLLOUT_TREES, 1), 70, 101)
    light_level = jax.random.randint(jax.random.fold_in(key, 38), (ROLLOUT_TREES, 1), 10, 31)
    fill_level = jnp.where(side_of_tree == 1, heavy_level, light_level)
    roll_value = jax.random.randint(jax.random.fold_in(key, 32), (ROLLOUT_TREES, BRANCH_SLOTS), 0, 100)
    branch_size = jax.random.randint(jax.random.fold_in(key, 33), (ROLLOUT_TREES, BRANCH_SLOTS), 1, TILE_ROWS + 1)
    found = jnp.where(roll_value < fill_level, branch_size, 0)
    pair_index = jax.random.randint(jax.random.fold_in(key, 34), (), 0, half_trees)
    column = jax.random.randint(jax.random.fold_in(key, 35), (), 0, BRANCH_SLOTS // TILES_DEV)
    flip_side = jax.random.randint(jax.random.fold_in(key, 36), (), 0, 2)
    giver_tree = pair_index + flip_side * half_trees
    taker_tree = pair_index + (1 - flip_side) * half_trees
    branch_ids = jnp.arange(BRANCH_SLOTS)[None, :]
    in_column = branch_ids // TILES_DEV == column
    found = jnp.where((tree_ids == giver_tree) & in_column, jnp.maximum(found, 1), found)
    found = jnp.where((tree_ids == taker_tree) & in_column, 0, found)
    found = jnp.where((tree_ids == giver_tree) & (branch_ids == column * TILES_DEV), TILE_ROWS, found)
    return found.astype(jnp.int32)


def place_ends(result, rng, least, largest):
    longest = result.shape.index(max(result.shape))
    spots = []
    for shift in (0, 1):
        where = [jax.random.randint(jax.random.fold_in(rng, axis), (), 0, length) for axis, length in enumerate(result.shape)]
        where[longest] = (where[longest] + shift) % result.shape[longest]
        spots.append(tuple(where))
    return result.at[spots[0]].set(least).at[spots[1]].set(largest)


def shard_levels(key, shape, shards, least, high):
    def one(position, parts):
        heights = jax.random.uniform(jax.random.fold_in(jax.random.fold_in(key, 6), position), (parts,), jnp.float32, least / len(shards), high / len(shards))
        return jnp.repeat(jnp.exp(heights), shape[position] // parts).reshape((-1,) + (1,) * (len(shape) - position - 1))

    loudness = one(*shards[0])
    for cut in shards[1:]:
        loudness = loudness * one(*cut)
    return loudness


def normal_values(own_key, extent, width, bound, shards=(), held_as=jnp.bfloat16):
    drawn = jax.random.normal(own_key, extent, jnp.float32) * width
    if len(shards) > 0:
        drawn = shard_levels(own_key, extent, shards, -0.22, 0.18) * drawn
    return jnp.clip(drawn, min=-bound, max=bound).astype(held_as)


def setup_inputs(seed: int = 0) -> dict:
    streams_of = jax.random.split(jax.random.key(seed), 9)
    queries = draw_queries(jax.random.fold_in(streams_of[8], 71), 0)
    branch_key_rows = normal_values(streams_of[1], (ROLLOUT_TREES, BRANCH_SLOTS * TILE_ROWS, KEY_VALUE_HEADS * HEAD_SIZE), 1.0, 6.0, ((0, 8), (1, 32)))
    branch_value_rows = normal_values(streams_of[2], (ROLLOUT_TREES, BRANCH_SLOTS * TILE_ROWS, KEY_VALUE_HEADS * HEAD_SIZE), 1.0, 6.0, ((0, 8), (1, 32)))
    grad_output = normal_values(streams_of[3], (ROLLOUT_TREES, BRANCH_SLOTS * TILE_ROWS, QUERY_HEADS * HEAD_SIZE), 1.0, 6.0, ((0, 8), (1, 32)))
    trunk_keys = draw_trunk_keys(jax.random.fold_in(streams_of[8], 71), 0)
    trunk_token_values = normal_values(streams_of[5], (ROLLOUT_TREES, TRUNK_TOKENS, KEY_VALUE_HEADS * HEAD_SIZE), 1.0, 6.0, ((0, 8), (1, 32)))
    lengths = draw_lengths(jax.random.fold_in(streams_of[8], 71), 0)
    parents = place_ends(jax.random.randint(streams_of[7], (ROLLOUT_TREES, BRANCH_SLOTS), 1, TRUNK_TOKENS), jax.random.fold_in(streams_of[7], 1), 1, TRUNK_TOKENS - 1).astype(jnp.int32)
    return {"queries": queries, "branch_key_rows": branch_key_rows, "branch_value_rows": branch_value_rows, "grad_output": grad_output, "trunk_keys": trunk_keys, "trunk_token_values": trunk_token_values, "lengths": lengths, "parents": parents}


masked_score = -1e+30

def tile_grads(tile_items):
    query_rows, grad_rows, key_rows, value_rows, trunk_keys_all, trunk_vals_all, length, parent = tile_items
    row_count = query_rows.shape[0]
    trunk_len = trunk_keys_all.shape[0]
    width_span = QUERY_HEADS // KEY_VALUE_HEADS * HEAD_SIZE
    score_scale = 1.0 / math.sqrt(HEAD_SIZE)
    all_keys = jnp.concatenate([trunk_keys_all, key_rows], axis=0).astype(jnp.float32)
    all_values = jnp.concatenate([trunk_vals_all, value_rows], axis=0).astype(jnp.float32)
    row_ids = lax.broadcasted_iota(jnp.int32, (row_count, trunk_len + row_count), 0)
    col_ids = lax.broadcasted_iota(jnp.int32, (row_count, trunk_len + row_count), 1)
    allowed = jnp.where(col_ids < trunk_len, col_ids <= parent, col_ids - trunk_len <= row_ids)
    live_rows = (lax.broadcasted_iota(jnp.int32, (row_count, 1), 0) < length).astype(jnp.float32)
    query_parts, key_parts, value_parts = ([], [], [])
    for index_of_head in range(KEY_VALUE_HEADS):
        query_head = query_rows[:, index_of_head * width_span:(index_of_head + 1) * width_span].astype(jnp.float32).reshape(row_count, width_span // HEAD_SIZE, HEAD_SIZE)
        grad_head = grad_rows[:, index_of_head * width_span:(index_of_head + 1) * width_span].astype(jnp.float32).reshape(row_count, width_span // HEAD_SIZE, HEAD_SIZE)
        key_head = all_keys[:, index_of_head * HEAD_SIZE:(index_of_head + 1) * HEAD_SIZE]
        value_head = all_values[:, index_of_head * HEAD_SIZE:(index_of_head + 1) * HEAD_SIZE]
        scores = jnp.einsum('igd,jd->gij', query_head, key_head, precision=lax.Precision.HIGHEST) * score_scale
        scores = jnp.where(allowed[None], scores, masked_score)
        row_peak = lax.optimization_barrier(jnp.max(scores, axis=-1, keepdims=True))
        exponent = jnp.where(allowed[None], jnp.exp(scores - row_peak), 0.0)
        weights = exponent / lax.optimization_barrier(jnp.sum(exponent, axis=-1, keepdims=True)) * live_rows[None]
        weights_low = weights.astype(jnp.bfloat16).astype(jnp.float32)
        grad_weights = jnp.einsum('igd,jd->gij', grad_head, value_head, precision=lax.Precision.HIGHEST)
        row_delta = lax.optimization_barrier(jnp.sum(weights * grad_weights, axis=-1, keepdims=True))
        dscore = (weights * (grad_weights - row_delta) * score_scale).astype(jnp.bfloat16).astype(jnp.float32)
        query_parts.append(jnp.einsum('gij,jd->igd', dscore, key_head, precision=lax.Precision.HIGHEST).reshape(row_count, width_span))
        key_parts.append(jnp.einsum('gij,igd->jd', dscore, query_head, precision=lax.Precision.HIGHEST))
        value_parts.append(jnp.einsum('gij,igd->jd', weights_low, grad_head, precision=lax.Precision.HIGHEST))
    return (jnp.concatenate(query_parts, axis=1), jnp.concatenate(key_parts, axis=1), jnp.concatenate(value_parts, axis=1))

def skipped(tile_items):
    row_count = tile_items[0].shape[0]
    total = tile_items[4].shape[0] + row_count
    return (jnp.zeros((row_count, tile_items[0].shape[1]), jnp.float32), jnp.zeros((total, tile_items[2].shape[1]), jnp.float32), jnp.zeros((total, tile_items[2].shape[1]), jnp.float32))

def one_tree(tree_items):
    query_full, gradient_full, key_full, value_full, trunk_keys_all, trunk_vals_all, length_per_tree, parent_per_tree = tree_items

    def one_tile(partial_sums, slot_entries):
        query_rows, grad_rows, key_rows, value_rows, length, parent = slot_entries
        results = lax.cond(length > 0, tile_grads, skipped, (query_rows, grad_rows, key_rows, value_rows, trunk_keys_all, trunk_vals_all, length, parent))
        new_sums = (partial_sums[0] + results[1][:TRUNK_TOKENS], partial_sums[1] + results[2][:TRUNK_TOKENS])
        return (new_sums, (results[0], results[1][TRUNK_TOKENS:], results[2][TRUNK_TOKENS:]))
    initial_sums = (jnp.zeros((TRUNK_TOKENS, KEY_VALUE_HEADS * HEAD_SIZE), jnp.float32), jnp.zeros((TRUNK_TOKENS, KEY_VALUE_HEADS * HEAD_SIZE), jnp.float32))
    slot_entries = (query_full.reshape(BRANCH_SLOTS, TILE_ROWS, QUERY_HEADS * HEAD_SIZE), gradient_full.reshape(BRANCH_SLOTS, TILE_ROWS, QUERY_HEADS * HEAD_SIZE), key_full.reshape(BRANCH_SLOTS, TILE_ROWS, KEY_VALUE_HEADS * HEAD_SIZE), value_full.reshape(BRANCH_SLOTS, TILE_ROWS, KEY_VALUE_HEADS * HEAD_SIZE), length_per_tree, parent_per_tree)
    trunk_partial_sums, tile_outputs = lax.scan(one_tile, initial_sums, slot_entries)
    return (tile_outputs[0].reshape(BRANCH_SLOTS * TILE_ROWS, QUERY_HEADS * HEAD_SIZE), tile_outputs[1].reshape(BRANCH_SLOTS * TILE_ROWS, KEY_VALUE_HEADS * HEAD_SIZE), tile_outputs[2].reshape(BRANCH_SLOTS * TILE_ROWS, KEY_VALUE_HEADS * HEAD_SIZE), trunk_partial_sums[0], trunk_partial_sums[1])

def reference(queries, branch_key_rows, branch_value_rows, grad_output, trunk_keys, trunk_token_values, lengths, parents):
    results = lax.map(one_tree, (queries, grad_output, branch_key_rows, branch_value_rows, trunk_keys, trunk_token_values, lengths, parents))
    return (results[0], results[1], results[2], results[3], results[4])
```

```python
import math

import jax
import jax.numpy as jnp
from jax import lax
from jax.experimental import pallas as pl
from jax.experimental.pallas import tpu as pltpu
from jax.sharding import PartitionSpec as P

HEAD_SIZE = 128
MASKED = -1e30
CHUNK = 256


def dot_nt(a, b):
    return lax.dot_general(a, b, (((1,), (1,)), ((), ())), preferred_element_type=jnp.float32)


def dot_tn(a, b):
    return lax.dot_general(a, b, (((0,), (0,)), ((), ())), preferred_element_type=jnp.float32)


def dot_nn(a, b):
    return lax.dot_general(a, b, (((1,), (0,)), ((), ())), preferred_element_type=jnp.float32)


def lanes(start):
    if isinstance(start, int):
        return slice(start, start + HEAD_SIZE)
    return pl.ds(pl.multiple_of(start, HEAD_SIZE), HEAD_SIZE)


def iota(shape, dim):
    return lax.broadcasted_iota(jnp.int32, shape, dim)


def score_kernel(
    leaf,
    lengths,
    parents,
    q_hbm,
    do_hbm,
    kv,
    kb_hbm,
    vb_hbm,
    sums,
    ds_hbm,
    pb_hbm,
    kv_hbm,
    q,
    do,
    kb,
    vb,
    ds_buf,
    pb_buf,
    key_mask,
    sems_in,
    sems_out,
    *,
    tiles,
):
    rows = q_hbm.shape[0] // tiles
    trunk = kv.shape[0]
    width = kb.shape[1]
    heads = width // HEAD_SIZE
    group_width = q_hbm.shape[1] // heads

    def fetches(h):
        span = pl.ds(pl.multiple_of(h * group_width, group_width), group_width)
        return [
            pltpu.make_async_copy(q_hbm.at[:, span], q.at[h], sems_in.at[0, h]),
            pltpu.make_async_copy(do_hbm.at[:, span], do.at[h], sems_in.at[1, h]),
        ]

    def stores(h):
        return [
            pltpu.make_async_copy(ds_buf.at[:, h], ds_hbm.at[:, h], sems_out.at[0, h]),
            pltpu.make_async_copy(pb_buf.at[:, h], pb_hbm.at[:, h], sems_out.at[1, h]),
        ]

    branch_fetches = [
        pltpu.make_async_copy(kb_hbm, kb, sems_in.at[0, heads]),
        pltpu.make_async_copy(vb_hbm, vb, sems_in.at[1, heads]),
    ]
    kv_store = pltpu.make_async_copy(kv, kv_hbm, sems_out.at[0, heads])
    for copy in fetches(0) + branch_fetches:
        copy.start()
    for h in range(1, heads):
        for copy in fetches(h):
            copy.start()
    kv_store.start()
    per_chunk = CHUNK // rows
    chunk_width = per_chunk * HEAD_SIZE
    halves = group_width // chunk_width
    scale = 1.0 / math.sqrt(HEAD_SIZE)
    to_exp2 = scale * math.log2(math.e)
    tree = leaf[0]

    shape = (CHUNK, HEAD_SIZE)
    column, row = iota(shape, 1), jnp.bitwise_and(iota(shape, 0), rows - 1)
    query_mask = jnp.where(
        column < rows,
        jnp.where(column > row, MASKED, 0.0),
        jnp.where(column == rows, 1.0, 0.0),
    ).astype(jnp.bfloat16)
    shape = (trunk + rows, HEAD_SIZE)
    column, row = iota(shape, 1), iota(shape, 0)
    branch_part = jnp.where(row == column + trunk, 1.0, 0.0)
    for t in range(tiles):
        key_mask[t] = jnp.where(
            (column == rows) & (row > parents[tree, t]) & (row < trunk),
            MASKED,
            jnp.where(column < rows, branch_part, 0.0),
        ).astype(jnp.bfloat16)
    lane_row = jnp.bitwise_and(iota((1, CHUNK), 1), rows - 1)
    live = [jnp.where(lane_row < lengths[tree, t], 1.0, 0.0) for t in range(tiles)]

    for copy in branch_fetches:
        copy.wait()

    def head_step(h, carry):
        for copy in fetches(h):
            copy.wait()

        def stacked(ref, t, half):
            first = half * chunk_width
            return jnp.concatenate(
                [
                    ref[h, t * rows : (t + 1) * rows, lanes(first + j * HEAD_SIZE)]
                    for j in range(per_chunk)
                ],
                axis=0,
            )

        trunk_keys = kv[:, lanes(h * HEAD_SIZE)]
        trunk_vals = kv[:, lanes(width + h * HEAD_SIZE)]

        def matmuls(c):
            t, half = c // halves, c % halves
            tile = slice(t * rows, (t + 1) * rows)
            queries, grads = stacked(q, t, half), stacked(do, t, half)
            keys = jnp.concatenate([trunk_keys, kb[tile, lanes(h * HEAD_SIZE)]], axis=0)
            values = jnp.concatenate([trunk_vals, vb[tile, lanes(h * HEAD_SIZE)]], axis=0)
            scores = dot_nt(
                jnp.concatenate([keys, key_mask[t]], axis=1),
                jnp.concatenate([queries, query_mask], axis=1),
            )
            return scores, dot_nt(values, grads), queries, grads

        def softmax(c, scores, grad_weights):
            t, half = c // halves, c % halves
            peak = jnp.max(scores, axis=0, keepdims=True)
            e = jnp.exp2((scores - peak) * to_exp2)
            inv = live[t] / jnp.sum(e, axis=0, keepdims=True)
            delta = inv * jnp.sum(e * grad_weights, axis=0, keepdims=True)
            weights = e * inv
            low = weights.astype(jnp.bfloat16)
            ds = (weights * (grad_weights - delta)).astype(jnp.bfloat16)
            part = slice(half * CHUNK, (half + 1) * CHUNK)
            ds_buf[t, h, :, part] = ds
            pb_buf[t, h, :, part] = low[trunk:]
            return ds[:trunk], low[:trunk]

        chunks = tiles * halves
        key_sum = value_sum = None
        ahead = matmuls(0)
        for c in range(chunks):
            scores, grad_weights, queries, grads = ahead
            if c + 1 < chunks:
                ahead = matmuls(c + 1)
            ds, low = softmax(c, scores, grad_weights)
            key_part, value_part = dot_nn(ds, queries), dot_nn(low, grads)
            key_sum = key_part if c == 0 else key_sum + key_part
            value_sum = value_part if c == 0 else value_sum + value_part
        shape = (sums.shape[0], sums.shape[2], HEAD_SIZE)
        sums[:, 0, :, lanes(h * HEAD_SIZE)] = (
            (key_sum * scale).reshape(shape).astype(jnp.bfloat16)
        )
        sums[:, 1, :, lanes(h * HEAD_SIZE)] = value_sum.reshape(shape).astype(jnp.bfloat16)
        for copy in stores(h):
            copy.start()
        return carry

    lax.fori_loop(0, heads, head_step, 0)
    kv_store.wait()
    for h in range(heads):
        for copy in stores(h):
            copy.wait()


def grad_kernel(
    q_hbm,
    do_hbm,
    kv,
    kb_hbm,
    ds_hbm,
    pb_hbm,
    dq,
    dkb,
    dvb,
    q,
    do,
    kb,
    ds,
    pb,
    dq_buf,
    dkb_buf,
    dvb_buf,
    sems_in,
    sems,
    *,
    tiles,
):
    rows = q_hbm.shape[0] // tiles
    trunk = kv.shape[0]
    heads = kb.shape[1] // HEAD_SIZE
    group_width = q.shape[1] // heads
    groups = group_width // HEAD_SIZE
    scale = 1.0 / math.sqrt(HEAD_SIZE)

    def fetches(t):
        tile = pl.ds(pl.multiple_of(t * rows, rows), rows)
        return [
            pltpu.make_async_copy(source.at[part], buf.at[part], sems_in.at[i, t])
            for i, (source, buf, part) in enumerate(
                (
                    (ds_hbm, ds, t),
                    (q_hbm, q, tile),
                    (do_hbm, do, tile),
                    (pb_hbm, pb, t),
                    (kb_hbm, kb, tile),
                )
            )
        ]

    for t in range(tiles):
        for copy in fetches(t):
            copy.start()

    def copies(t):
        tile = pl.ds(pl.multiple_of(t * rows, rows), rows)
        return [
            pltpu.make_async_copy(buf.at[tile], out.at[tile], sems.at[i, t])
            for i, (buf, out) in enumerate(((dq_buf, dq), (dkb_buf, dkb), (dvb_buf, dvb)))
        ]

    def tile_step(t, carry):
        for copy in fetches(t):
            copy.wait()
        tile = pl.ds(pl.multiple_of(t * rows, rows), rows)

        def stacked(ref, h):
            return jnp.concatenate(
                [ref[tile, lanes(h * group_width + j * HEAD_SIZE)] for j in range(groups)], axis=0
            )

        for h in range(heads):
            span = lanes(h * HEAD_SIZE)
            keys = jnp.concatenate([kv[:, span], kb[tile, span]], axis=0)
            dkb_buf[tile, span] = dot_nn(ds[t, h, trunk:, :], stacked(q, h)) * scale
            dvb_buf[tile, span] = dot_nn(pb[t, h], stacked(do, h))
            got = (dot_tn(keys, ds[t, h]) * scale).T
            for j in range(groups):
                dq_buf[tile, lanes(h * group_width + j * HEAD_SIZE)] = got[
                    j * rows : (j + 1) * rows
                ]
        for copy in copies(t):
            copy.start()
        return carry

    lax.fori_loop(0, tiles, tile_step, 0)
    for t in range(tiles):
        for copy in copies(t):
            copy.wait()


def per_device(
    queries,
    branch_key_rows,
    branch_value_rows,
    grad_output,
    trunk_keys,
    trunk_token_values,
    lengths,
    parents,
):
    q = queries[0]
    do = grad_output[0]
    kb = branch_key_rows[0]
    vb = branch_value_rows[0]
    seq = lax.axis_size("seq")
    leaf = lax.axis_index("leaf").astype(jnp.int32).reshape(1)
    tiles = lengths.shape[1]
    rows = q.shape[0] // tiles
    width = kb.shape[1]
    heads = width // HEAD_SIZE
    wide = q.shape[1] // width * rows
    own = trunk_keys.shape[1]
    trunk = own * seq
    work = heads * tiles * wide * (trunk + rows) * HEAD_SIZE * 2

    both = jnp.concatenate([trunk_keys[0], trunk_token_values[0]], axis=1)
    spread = jnp.broadcast_to(both[None], (seq,) + both.shape)
    gathered = lax.all_to_all(spread, "seq", 0, 0, tiled=True).reshape(trunk, 2 * width)

    vmem = pl.BlockSpec(memory_space=pltpu.VMEM)
    smem = pl.BlockSpec(memory_space=pltpu.SMEM)
    hbm = pl.BlockSpec(memory_space=pltpu.HBM)
    ds_shape = (tiles, heads, trunk + rows, wide)
    pb_shape = (tiles, heads, rows, wide)
    head_shape = (heads, tiles * rows, q.shape[1] // heads)

    sums, ds, pb, kv = pl.pallas_call(
        lambda *refs: score_kernel(*refs, tiles=tiles),
        in_specs=[smem] * 3 + [hbm, hbm, vmem, hbm, hbm],
        out_specs=[vmem, hbm, hbm, hbm],
        out_shape=[
            jax.ShapeDtypeStruct((seq, 2, own, width), jnp.bfloat16),
            jax.ShapeDtypeStruct(ds_shape, jnp.bfloat16),
            jax.ShapeDtypeStruct(pb_shape, jnp.bfloat16),
            jax.ShapeDtypeStruct(gathered.shape, jnp.bfloat16),
        ],
        scratch_shapes=[
            pltpu.VMEM(head_shape, jnp.bfloat16),
            pltpu.VMEM(head_shape, jnp.bfloat16),
            pltpu.VMEM(kb.shape, jnp.bfloat16),
            pltpu.VMEM(vb.shape, jnp.bfloat16),
            pltpu.VMEM(ds_shape, jnp.bfloat16),
            pltpu.VMEM(pb_shape, jnp.bfloat16),
            pltpu.VMEM((tiles, trunk + rows, HEAD_SIZE), jnp.bfloat16),
            pltpu.SemaphoreType.DMA((2, heads + 1)),
            pltpu.SemaphoreType.DMA((2, heads + 1)),
        ],
        compiler_params=pltpu.CompilerParams(vmem_limit_bytes=65_900_000),
        cost_estimate=pl.CostEstimate(
            flops=4 * work, bytes_accessed=12 << 20, transcendentals=work // 256
        ),
        name="scores",
    )(leaf, lengths, parents, q, do, gathered, kb, vb)

    shares = lax.all_to_all(sums, "seq", 0, 0, tiled=True)

    dq, dkb, dvb = pl.pallas_call(
        lambda *refs: grad_kernel(*refs, tiles=tiles),
        in_specs=[hbm, hbm, vmem, hbm, hbm, hbm],
        out_specs=[hbm] * 3,
        out_shape=[
            jax.ShapeDtypeStruct(q.shape, jnp.float32),
            jax.ShapeDtypeStruct(kb.shape, jnp.float32),
            jax.ShapeDtypeStruct(vb.shape, jnp.float32),
        ],
        scratch_shapes=[
            pltpu.VMEM(q.shape, jnp.bfloat16),
            pltpu.VMEM(q.shape, jnp.bfloat16),
            pltpu.VMEM(kb.shape, jnp.bfloat16),
            pltpu.VMEM(ds_shape, jnp.bfloat16),
            pltpu.VMEM(pb_shape, jnp.bfloat16),
            pltpu.VMEM(q.shape, jnp.float32),
            pltpu.VMEM(kb.shape, jnp.float32),
            pltpu.VMEM(vb.shape, jnp.float32),
            pltpu.SemaphoreType.DMA((5, tiles)),
            pltpu.SemaphoreType.DMA((3, tiles)),
        ],
        compiler_params=pltpu.CompilerParams(vmem_limit_bytes=65_900_000),
        cost_estimate=pl.CostEstimate(flops=2 * work, bytes_accessed=16 << 20, transcendentals=0),
        name="grads",
    )(q, do, kv, kb, ds, pb)

    trunk_grads = jnp.sum(shares.astype(jnp.float32), axis=0)
    return dq[None], dkb[None], dvb[None], trunk_grads[0][None], trunk_grads[1][None]


def solution(mesh):
    split = P("leaf", "seq", None)
    return jax.shard_map(
        per_device,
        mesh=mesh,
        in_specs=(split,) * 6 + (P(None, "seq"),) * 2,
        out_specs=(split,) * 5,
        check_vma=False,
    )
```

```python
import math

import jax
import jax.numpy as jnp
from jax import lax
from jax.experimental import pallas as pl
from jax.experimental.pallas import tpu as pltpu
from jax.sharding import PartitionSpec as P

HEAD_SIZE = 128
MASKED = -1e30
CHUNK = 256


def dot_nt(a, b):
    return lax.dot_general(a, b, (((1,), (1,)), ((), ())), preferred_element_type=jnp.float32)


def dot_tn(a, b):
    return lax.dot_general(a, b, (((0,), (0,)), ((), ())), preferred_element_type=jnp.float32)


def dot_nn(a, b):
    return lax.dot_general(a, b, (((1,), (0,)), ((), ())), preferred_element_type=jnp.float32)


def lanes(start):
    if isinstance(start, int):
        return slice(start, start + HEAD_SIZE)
    return pl.ds(pl.multiple_of(start, HEAD_SIZE), HEAD_SIZE)


def iota(shape, dim):
    return lax.broadcasted_iota(jnp.int32, shape, dim)


def stacked(ref, h, tile, first, count):
    return jnp.concatenate(
        [ref[h, tile, lanes((first + j) * HEAD_SIZE)] for j in range(count)], axis=0
    )


def head_fetches(h, q_hbm, do_hbm, q, do, sems):
    width = q.shape[2]
    span = pl.ds(pl.multiple_of(h * width, width), width)
    return [
        pltpu.make_async_copy(q_hbm.at[:, span], q.at[h], sems.at[0, h]),
        pltpu.make_async_copy(do_hbm.at[:, span], do.at[h], sems.at[1, h]),
    ]


def mask_of_queries(rows):
    shape = (CHUNK, HEAD_SIZE)
    column, row = iota(shape, 1), jnp.bitwise_and(iota(shape, 0), rows - 1)
    return jnp.where(
        column < rows,
        jnp.where(column > row, MASKED, 0.0),
        jnp.where(column == rows, 1.0, 0.0),
    ).astype(jnp.bfloat16)


def local_kernel(
    q_hbm,
    do_hbm,
    kb_hbm,
    vb_hbm,
    e_hbm,
    g_hbm,
    stats_hbm,
    q,
    do,
    kb,
    vb,
    e_buf,
    g_buf,
    stats,
    query_mask,
    sems_in,
    sems_out,
    *,
    tiles,
):
    rows = q_hbm.shape[0] // tiles
    heads = q.shape[0]
    per_chunk = CHUNK // rows
    halves = q.shape[2] // (per_chunk * HEAD_SIZE)
    to_exp2 = math.log2(math.e) / math.sqrt(HEAD_SIZE)
    branch_fetches = [
        pltpu.make_async_copy(kb_hbm, kb, sems_in.at[0, heads]),
        pltpu.make_async_copy(vb_hbm, vb, sems_in.at[1, heads]),
    ]
    for copy in branch_fetches:
        copy.start()
    for h in range(heads):
        for copy in head_fetches(h, q_hbm, do_hbm, q, do, sems_in):
            copy.start()
    query_mask[...] = mask_of_queries(rows)
    shape = (rows, HEAD_SIZE)
    one_hot = jnp.where(iota(shape, 0) == iota(shape, 1), 1.0, 0.0).astype(jnp.bfloat16)
    for copy in branch_fetches:
        copy.wait()

    def stores(h):
        used = slice(0, stats.shape[2])
        return [
            pltpu.make_async_copy(e_buf.at[:, h], e_hbm.at[:, h], sems_out.at[0, h]),
            pltpu.make_async_copy(g_buf.at[:, h], g_hbm.at[:, h], sems_out.at[1, h]),
            pltpu.make_async_copy(stats.at[:, h], stats_hbm.at[:, h, used], sems_out.at[2, h]),
        ]

    def head_step(h, carry):
        for copy in head_fetches(h, q_hbm, do_hbm, q, do, sems_in):
            copy.wait()
        span = lanes(h * HEAD_SIZE)
        for t in range(tiles):
            tile = slice(t * rows, (t + 1) * rows)
            for half in range(halves):
                queries = stacked(q, h, tile, half * per_chunk, per_chunk)
                grads = stacked(do, h, tile, half * per_chunk, per_chunk)
                score = dot_nt(
                    jnp.concatenate([kb[tile, span], one_hot], axis=1),
                    jnp.concatenate([queries, query_mask[...]], axis=1),
                )
                grad = dot_nt(vb[tile, span], grads)
                peak = jnp.max(score, axis=0, keepdims=True)
                e = jnp.exp2((score - peak) * to_exp2)
                part = slice(half * CHUNK, (half + 1) * CHUNK)
                e_buf[t, h, :, part] = e.astype(jnp.bfloat16)
                g_buf[t, h, :, part] = grad.astype(jnp.bfloat16)
                stats[t, h, 0:1, part] = peak
                stats[t, h, 1:2, part] = jnp.sum(e, axis=0, keepdims=True)
                stats[t, h, 2:3, part] = jnp.sum(e * grad, axis=0, keepdims=True)
                stats[t, h, 3:, part] = jnp.zeros((stats.shape[2] - 3, CHUNK), jnp.float32)
        for copy in stores(h):
            copy.start()
        return carry

    lax.fori_loop(0, heads, head_step, 0)
    for h in range(heads):
        for copy in stores(h):
            copy.wait()


def score_kernel(
    leaf,
    lengths,
    parents,
    q_hbm,
    do_hbm,
    kv,
    stats_hbm,
    sums_hbm,
    ds_hbm,
    rows_hbm,
    q,
    do,
    stats,
    sums,
    ds_buf,
    row_buf,
    low_buf,
    key_mask,
    query_mask,
    sems_in,
    sems_out,
    *,
    tiles,
):
    rows = q_hbm.shape[0] // tiles
    trunk = kv.shape[0]
    width = kv.shape[1] // 2
    heads = width // HEAD_SIZE
    group_width = q_hbm.shape[1] // heads
    per_chunk = CHUNK // rows
    halves = group_width // (per_chunk * HEAD_SIZE)
    scale = 1.0 / math.sqrt(HEAD_SIZE)
    to_exp2 = scale * math.log2(math.e)
    tree = leaf[0]

    def fetches(h):
        return head_fetches(h, q_hbm, do_hbm, q, do, sems_in)

    def tile_stores(h, t):
        return [
            pltpu.make_async_copy(ds_buf.at[t, h], ds_hbm.at[t * heads + h], sems_out.at[0, h, t]),
            pltpu.make_async_copy(
                row_buf.at[t, h],
                rows_hbm.at[t, h, 0 : row_buf.shape[2]],
                sems_out.at[1, h, t],
            ),
        ]

    def sum_store(h):
        span = lanes(h * HEAD_SIZE)
        return pltpu.make_async_copy(
            sums.at[h], sums_hbm.at[:, :, :, span], sems_out.at[2, h, 0]
        )

    kv_stores = [
        pltpu.make_async_copy(
            kv.at[:, i * width : (i + 1) * width],
            ds_hbm.at[tiles * heads + i],
            sems_out.at[2, i, 1],
        )
        for i in range(2)
    ]
    stats_fetch = pltpu.make_async_copy(
        stats_hbm.at[:, :, 0 : stats.shape[2]], stats, sems_in.at[0, heads]
    )
    for copy in fetches(0):
        copy.start()
    stats_fetch.start()
    for copy in kv_stores:
        copy.start()

    query_mask[...] = mask_of_queries(rows)
    shape = (trunk, HEAD_SIZE)
    column, row = iota(shape, 1), iota(shape, 0)
    for t in range(tiles):
        key_mask[t] = jnp.where(
            (column == rows) & (row > parents[tree, t]), MASKED, 0.0
        ).astype(jnp.bfloat16)
    lane_row = jnp.bitwise_and(iota((1, CHUNK), 1), rows - 1)
    live = [jnp.where(lane_row < lengths[tree, t], 1.0, 0.0) for t in range(tiles)]

    stats_fetch.wait()

    def matmuls(h, t, half):
        tile = slice(t * rows, (t + 1) * rows)
        queries = stacked(q, h, tile, half * per_chunk, per_chunk)
        grads = stacked(do, h, tile, half * per_chunk, per_chunk)
        scores = dot_nt(
            jnp.concatenate([kv[:, lanes(h * HEAD_SIZE)], key_mask[t]], axis=1),
            jnp.concatenate([queries, query_mask[...]], axis=1),
        )
        return scores, dot_nt(kv[:, lanes(width + h * HEAD_SIZE)], grads)

    def softmax(h, t, half, score, grad):
        part = slice(half * CHUNK, (half + 1) * CHUNK)
        branch_peak = stats[t, h, 0:1, part]
        peak = jnp.maximum(jnp.max(score, axis=0, keepdims=True), branch_peak)
        e = jnp.exp2((score - peak) * to_exp2)
        shrink = jnp.exp2((branch_peak - peak) * to_exp2)
        inv = live[t] / (jnp.sum(e, axis=0, keepdims=True) + shrink * stats[t, h, 1:2, part])
        delta = inv * (
            jnp.sum(e * grad, axis=0, keepdims=True) + shrink * stats[t, h, 2:3, part]
        )
        weights = e * inv
        ds_buf[t, h, :, part] = (weights * (grad - delta)).astype(jnp.bfloat16)
        low_buf[t, :, part] = weights.astype(jnp.bfloat16)
        row_buf[t, h, 0:1, part] = shrink * inv
        row_buf[t, h, 1:2, part] = delta
        row_buf[t, h, 2:, part] = jnp.zeros((row_buf.shape[2] - 2, CHUNK), jnp.float32)

    def trunk_parts(h, t):
        count = per_chunk * halves
        tile = slice(t * rows, (t + 1) * rows)
        left = jnp.concatenate([ds_buf[t, h], low_buf[t]], axis=0)
        right = jnp.concatenate(
            [stacked(q, h, tile, 0, count), stacked(do, h, tile, 0, count)], axis=1
        )
        both = dot_nn(left, right)
        return both[:trunk, :HEAD_SIZE], both[trunk:, HEAD_SIZE:]

    order = [(t, half) for t in range(tiles) for half in range(halves)]

    def head_step(h, carry):
        totals = None
        for copy in fetches(h):
            copy.wait()

        @pl.when(h + 1 < heads)
        def _():
            for copy in fetches(h + 1):
                copy.start()

        ahead = matmuls(h, *order[0])
        for c, (t, half) in enumerate(order):
            now = ahead
            if c + 1 < len(order):
                ahead = matmuls(h, *order[c + 1])
            softmax(h, t, half, *now)
            if half == halves - 1:
                parts = trunk_parts(h, t)
                totals = parts if t == 0 else tuple(a + b for a, b in zip(totals, parts))
                for copy in tile_stores(h, t):
                    copy.start()
        shape = (sums.shape[1], sums.shape[3], HEAD_SIZE)
        sums[h, :, 0] = (totals[0] * scale).reshape(shape).astype(jnp.bfloat16)
        sums[h, :, 1] = totals[1].reshape(shape).astype(jnp.bfloat16)
        sum_store(h).start()
        return carry

    lax.fori_loop(0, heads, head_step, 0)
    for copy in kv_stores:
        copy.wait()
    for h in range(heads):
        sum_store(h).wait()
        for t in range(tiles):
            for copy in tile_stores(h, t):
                copy.wait()


def grad_kernel(
    q_hbm,
    do_hbm,
    kb_hbm,
    ds_hbm,
    e_hbm,
    g_hbm,
    rows_hbm,
    dq,
    dkb,
    dvb,
    q,
    do,
    kv,
    kb,
    ds,
    e,
    g,
    row_values,
    dq_buf,
    dkb_buf,
    dvb_buf,
    sems_in,
    sems,
    *,
    tiles,
):
    rows = q_hbm.shape[0] // tiles
    width = kb_hbm.shape[1]
    heads = width // HEAD_SIZE
    group_width = q_hbm.shape[1] // heads
    groups = group_width // HEAD_SIZE
    scale = 1.0 / math.sqrt(HEAD_SIZE)

    def fetches(t):
        tile = pl.ds(pl.multiple_of(t * rows, rows), rows)
        return [
            pltpu.make_async_copy(source.at[part], buf.at[part], sems_in.at[i, t])
            for i, (source, buf, part) in enumerate(
                (
                    (q_hbm, q, tile),
                    (do_hbm, do, tile),
                    (e_hbm, e, t),
                    (g_hbm, g, t),
                    (kb_hbm, kb, tile),
                )
            )
        ]

    kv_fetches = [
        pltpu.make_async_copy(
            ds_hbm.at[tiles * heads + i],
            kv.at[:, i * width : (i + 1) * width],
            sems_in.at[7, i],
        )
        for i in range(2)
    ]
    for copy in kv_fetches:
        copy.start()
    def computed_fetches(t):
        return [
            pltpu.make_async_copy(
                ds_hbm.at[pl.ds(pl.multiple_of(t * heads, heads), heads)],
                ds.at[t],
                sems_in.at[5, t],
            ),
            pltpu.make_async_copy(
                rows_hbm.at[t, :, 0 : row_values.shape[2]], row_values.at[t], sems_in.at[6, t]
            ),
        ]

    for t in range(tiles):
        for copy in fetches(t) + computed_fetches(t):
            copy.start()
    for copy in kv_fetches:
        copy.wait()

    def copies(t):
        tile = pl.ds(pl.multiple_of(t * rows, rows), rows)
        return [
            pltpu.make_async_copy(buf.at[tile], out.at[tile], sems.at[i, t])
            for i, (buf, out) in enumerate(((dq_buf, dq), (dkb_buf, dkb), (dvb_buf, dvb)))
        ]

    def tile_step(t, carry):
        for copy in fetches(t) + computed_fetches(t):
            copy.wait()
        tile = pl.ds(pl.multiple_of(t * rows, rows), rows)

        def all_heads(ref, h):
            return jnp.concatenate(
                [ref[tile, lanes(h * group_width + j * HEAD_SIZE)] for j in range(groups)], axis=0
            )

        for h in range(heads):
            span = lanes(h * HEAD_SIZE)
            keys = jnp.concatenate([kv[:, span], kb[tile, span]], axis=0)
            weights = e[t, h].astype(jnp.float32) * row_values[t, h, 0:1, :]
            branch_ds = weights * (g[t, h].astype(jnp.float32) - row_values[t, h, 1:2, :])
            branch_ds = branch_ds.astype(jnp.bfloat16)
            dkb_buf[tile, span] = dot_nn(branch_ds, all_heads(q, h)) * scale
            dvb_buf[tile, span] = dot_nn(weights.astype(jnp.bfloat16), all_heads(do, h))
            got = (dot_tn(keys, jnp.concatenate([ds[t, h], branch_ds], axis=0)) * scale).T
            for j in range(groups):
                dq_buf[tile, lanes(h * group_width + j * HEAD_SIZE)] = got[
                    j * rows : (j + 1) * rows
                ]
        for copy in copies(t):
            copy.start()
        return carry

    lax.fori_loop(0, tiles, tile_step, 0)
    for t in range(tiles):
        for copy in copies(t):
            copy.wait()


def per_device(
    queries,
    branch_key_rows,
    branch_value_rows,
    grad_output,
    trunk_keys,
    trunk_token_values,
    lengths,
    parents,
):
    q = queries[0]
    do = grad_output[0]
    kb = branch_key_rows[0]
    vb = branch_value_rows[0]
    seq = lax.axis_size("seq")
    leaf = lax.axis_index("leaf").astype(jnp.int32).reshape(1)
    tiles = lengths.shape[1]
    rows = q.shape[0] // tiles
    width = kb.shape[1]
    heads = width // HEAD_SIZE
    wide = q.shape[1] // width * rows
    own = trunk_keys.shape[1]
    trunk = own * seq
    work = heads * tiles * wide * (trunk + rows) * HEAD_SIZE * 2

    both = jnp.concatenate([trunk_keys[0], trunk_token_values[0]], axis=1)
    spread = jnp.broadcast_to(both[None], (seq,) + both.shape)
    gathered = lax.all_to_all(spread, "seq", 0, 0, tiled=True).reshape(trunk, 2 * width)

    vmem = pl.BlockSpec(memory_space=pltpu.VMEM)
    smem = pl.BlockSpec(memory_space=pltpu.SMEM)
    hbm = pl.BlockSpec(memory_space=pltpu.HBM)
    ds_shape = (tiles, heads, trunk, wide)
    branch_shape = (tiles, heads, rows, wide)
    stats_shape = (tiles, heads, 8, wide)
    kept_shape = (tiles, heads, rows + 16, wide)
    head_shape = (heads, tiles * rows, q.shape[1] // heads)

    e, g, stats = pl.pallas_call(
        lambda *refs: local_kernel(*refs, tiles=tiles),
        in_specs=[hbm] * 4,
        out_specs=[hbm] * 3,
        out_shape=[
            jax.ShapeDtypeStruct(branch_shape, jnp.bfloat16),
            jax.ShapeDtypeStruct(branch_shape, jnp.bfloat16),
            jax.ShapeDtypeStruct(kept_shape, jnp.float32),
        ],
        scratch_shapes=[
            pltpu.VMEM(head_shape, jnp.bfloat16),
            pltpu.VMEM(head_shape, jnp.bfloat16),
            pltpu.VMEM(kb.shape, jnp.bfloat16),
            pltpu.VMEM(vb.shape, jnp.bfloat16),
            pltpu.VMEM(branch_shape, jnp.bfloat16),
            pltpu.VMEM(branch_shape, jnp.bfloat16),
            pltpu.VMEM(stats_shape, jnp.float32),
            pltpu.VMEM((CHUNK, HEAD_SIZE), jnp.bfloat16),
            pltpu.SemaphoreType.DMA((2, heads + 1)),
            pltpu.SemaphoreType.DMA((3, heads)),
        ],
        compiler_params=pltpu.CompilerParams(vmem_limit_bytes=65_900_000),
        cost_estimate=pl.CostEstimate(flops=2 * work, bytes_accessed=7 << 20, transcendentals=0),
        name="local",
    )(q, do, kb, vb)

    sums, ds, row_values = pl.pallas_call(
        lambda *refs: score_kernel(*refs, tiles=tiles),
        in_specs=[smem] * 3 + [hbm, hbm, vmem, hbm],
        out_specs=[hbm] * 3,
        out_shape=[
            jax.ShapeDtypeStruct((seq, 2, own, width), jnp.bfloat16),
            jax.ShapeDtypeStruct((tiles * heads + 2, trunk, wide), jnp.bfloat16),
            jax.ShapeDtypeStruct(kept_shape, jnp.float32),
        ],
        scratch_shapes=[
            pltpu.VMEM(head_shape, jnp.bfloat16),
            pltpu.VMEM(head_shape, jnp.bfloat16),
            pltpu.VMEM(stats_shape, jnp.float32),
            pltpu.VMEM((heads, seq, 2, own, HEAD_SIZE), jnp.bfloat16),
            pltpu.VMEM(ds_shape, jnp.bfloat16),
            pltpu.VMEM(stats_shape, jnp.float32),
            pltpu.VMEM((tiles, trunk, wide), jnp.bfloat16),
            pltpu.VMEM((tiles, trunk, HEAD_SIZE), jnp.bfloat16),
            pltpu.VMEM((CHUNK, HEAD_SIZE), jnp.bfloat16),
            pltpu.SemaphoreType.DMA((2, heads + 1)),
            pltpu.SemaphoreType.DMA((3, heads, tiles)),
        ],
        compiler_params=pltpu.CompilerParams(vmem_limit_bytes=53_500_000),
        cost_estimate=pl.CostEstimate(
            flops=4 * work, bytes_accessed=12 << 20, transcendentals=work // 256
        ),
        name="scores",
    )(leaf, lengths, parents, q, do, gathered, stats)

    shares = lax.all_to_all(sums, "seq", 0, 0, tiled=True)

    dq, dkb, dvb = pl.pallas_call(
        lambda *refs: grad_kernel(*refs, tiles=tiles),
        in_specs=[hbm] * 7,
        out_specs=[hbm] * 3,
        out_shape=[
            jax.ShapeDtypeStruct(q.shape, jnp.float32),
            jax.ShapeDtypeStruct(kb.shape, jnp.float32),
            jax.ShapeDtypeStruct(vb.shape, jnp.float32),
        ],
        scratch_shapes=[
            pltpu.VMEM(q.shape, jnp.bfloat16),
            pltpu.VMEM(q.shape, jnp.bfloat16),
            pltpu.VMEM(gathered.shape, jnp.bfloat16),
            pltpu.VMEM(kb.shape, jnp.bfloat16),
            pltpu.VMEM(ds_shape, jnp.bfloat16),
            pltpu.VMEM(branch_shape, jnp.bfloat16),
            pltpu.VMEM(branch_shape, jnp.bfloat16),
            pltpu.VMEM(stats_shape, jnp.float32),
            pltpu.VMEM(q.shape, jnp.float32),
            pltpu.VMEM(kb.shape, jnp.float32),
            pltpu.VMEM(vb.shape, jnp.float32),
            pltpu.SemaphoreType.DMA((8, tiles)),
            pltpu.SemaphoreType.DMA((3, tiles)),
        ],
        compiler_params=pltpu.CompilerParams(vmem_limit_bytes=65_900_000),
        cost_estimate=pl.CostEstimate(flops=2 * work, bytes_accessed=16 << 20, transcendentals=0),
        name="grads",
    )(q, do, kb, ds, e, g, row_values)

    trunk_grads = jnp.sum(shares.astype(jnp.float32), axis=0)
    return dq[None], dkb[None], dvb[None], trunk_grads[0][None], trunk_grads[1][None]


def solution(mesh):
    split = P("leaf", "seq", None)
    return jax.shard_map(
        per_device,
        mesh=mesh,
        in_specs=(split,) * 6 + (P(None, "seq"),) * 2,
        out_specs=(split,) * 5,
        check_vma=False,
    )
```

```python
import math

import jax
import jax.numpy as jnp
from jax import lax
from jax.experimental import pallas as pl
from jax.experimental.pallas import tpu as pltpu
from jax.sharding import PartitionSpec as P

HEAD_SIZE = 128
MASKED = -1e30
CHUNK = 256


def dot_nt(a, b):
    return lax.dot_general(a, b, (((1,), (1,)), ((), ())), preferred_element_type=jnp.float32)


def dot_tn(a, b):
    return lax.dot_general(a, b, (((0,), (0,)), ((), ())), preferred_element_type=jnp.float32)


def dot_nn(a, b):
    return lax.dot_general(a, b, (((1,), (0,)), ((), ())), preferred_element_type=jnp.float32)


def lanes(start):
    if isinstance(start, int):
        return slice(start, start + HEAD_SIZE)
    return pl.ds(pl.multiple_of(start, HEAD_SIZE), HEAD_SIZE)


def iota(shape, dim):
    return lax.broadcasted_iota(jnp.int32, shape, dim)


def stacked(ref, h, tile, first, count):
    return jnp.concatenate(
        [ref[h, tile, lanes((first + j) * HEAD_SIZE)] for j in range(count)], axis=0
    )


def head_fetches(h, q_hbm, do_hbm, q, do, sems):
    width = q.shape[2]
    span = pl.ds(pl.multiple_of(h * width, width), width)
    return [
        pltpu.make_async_copy(q_hbm.at[:, span], q.at[h], sems.at[0, h]),
        pltpu.make_async_copy(do_hbm.at[:, span], do.at[h], sems.at[1, h]),
    ]


def mask_of_queries(rows):
    shape = (CHUNK, HEAD_SIZE)
    column, row = iota(shape, 1), jnp.bitwise_and(iota(shape, 0), rows - 1)
    return jnp.where(
        column < rows,
        jnp.where(column > row, MASKED, 0.0),
        jnp.where(column == rows, 1.0, 0.0),
    ).astype(jnp.bfloat16)


def local_kernel(
    q_hbm,
    do_hbm,
    kb_hbm,
    vb_hbm,
    e_hbm,
    g_hbm,
    stats_hbm,
    q,
    do,
    kb,
    vb,
    e_buf,
    g_buf,
    stats,
    query_mask,
    sems_in,
    sems_out,
    *,
    tiles,
):
    rows = q_hbm.shape[0] // tiles
    heads = q.shape[0]
    per_chunk = CHUNK // rows
    halves = q.shape[2] // (per_chunk * HEAD_SIZE)
    to_exp2 = math.log2(math.e) / math.sqrt(HEAD_SIZE)
    branch_fetches = [
        pltpu.make_async_copy(kb_hbm, kb, sems_in.at[0, heads]),
        pltpu.make_async_copy(vb_hbm, vb, sems_in.at[1, heads]),
    ]
    for copy in branch_fetches:
        copy.start()
    for h in range(heads):
        for copy in head_fetches(h, q_hbm, do_hbm, q, do, sems_in):
            copy.start()
    query_mask[...] = mask_of_queries(rows)
    shape = (rows, HEAD_SIZE)
    one_hot = jnp.where(iota(shape, 0) == iota(shape, 1), 1.0, 0.0).astype(jnp.bfloat16)
    for copy in branch_fetches:
        copy.wait()

    def stores(h):
        used = slice(0, stats.shape[2])
        return [
            pltpu.make_async_copy(e_buf.at[:, h], e_hbm.at[:, h], sems_out.at[0, h]),
            pltpu.make_async_copy(g_buf.at[:, h], g_hbm.at[:, h], sems_out.at[1, h]),
            pltpu.make_async_copy(stats.at[:, h], stats_hbm.at[:, h, used], sems_out.at[2, h]),
        ]

    def head_step(h, carry):
        for copy in head_fetches(h, q_hbm, do_hbm, q, do, sems_in):
            copy.wait()
        span = lanes(h * HEAD_SIZE)
        for t in range(tiles):
            tile = slice(t * rows, (t + 1) * rows)
            for half in range(halves):
                queries = stacked(q, h, tile, half * per_chunk, per_chunk)
                grads = stacked(do, h, tile, half * per_chunk, per_chunk)
                score = dot_nt(
                    jnp.concatenate([kb[tile, span], one_hot], axis=1),
                    jnp.concatenate([queries, query_mask[...]], axis=1),
                )
                grad = dot_nt(vb[tile, span], grads)
                peak = jnp.max(score, axis=0, keepdims=True)
                e = jnp.exp2((score - peak) * to_exp2)
                part = slice(half * CHUNK, (half + 1) * CHUNK)
                e_buf[t, h, :, part] = e.astype(jnp.bfloat16)
                g_buf[t, h, :, part] = grad.astype(jnp.bfloat16)
                stats[t, h, 0:1, part] = peak
                stats[t, h, 1:2, part] = jnp.sum(e, axis=0, keepdims=True)
                stats[t, h, 2:3, part] = jnp.sum(e * grad, axis=0, keepdims=True)
                stats[t, h, 3:, part] = jnp.zeros((stats.shape[2] - 3, CHUNK), jnp.float32)
        for copy in stores(h):
            copy.start()
        return carry

    lax.fori_loop(0, heads, head_step, 0)
    for h in range(heads):
        for copy in stores(h):
            copy.wait()


def score_kernel(
    leaf,
    lengths,
    parents,
    q_hbm,
    do_hbm,
    kv,
    stats_hbm,
    sums_hbm,
    ds_hbm,
    rows_hbm,
    q,
    do,
    stats,
    sums,
    ds_buf,
    row_buf,
    low_buf,
    key_mask,
    query_mask,
    sems_in,
    sems_out,
    *,
    tiles,
):
    rows = q_hbm.shape[0] // tiles
    trunk = kv.shape[0]
    width = kv.shape[1] // 2
    heads = width // HEAD_SIZE
    group_width = q_hbm.shape[1] // heads
    per_chunk = CHUNK // rows
    halves = group_width // (per_chunk * HEAD_SIZE)
    scale = 1.0 / math.sqrt(HEAD_SIZE)
    to_exp2 = scale * math.log2(math.e)
    tree = leaf[0]

    def fetches(h):
        return head_fetches(h, q_hbm, do_hbm, q, do, sems_in)

    def tile_stores(h, t):
        return [
            pltpu.make_async_copy(ds_buf.at[t, h], ds_hbm.at[t * heads + h], sems_out.at[0, h, t]),
            pltpu.make_async_copy(
                row_buf.at[t, h],
                rows_hbm.at[t, h, 0 : row_buf.shape[2]],
                sems_out.at[1, h, t],
            ),
        ]

    def sum_store(h):
        span = lanes(h * HEAD_SIZE)
        return pltpu.make_async_copy(
            sums.at[h], sums_hbm.at[:, :, :, span], sems_out.at[2, h, 0]
        )

    kv_stores = [
        pltpu.make_async_copy(
            kv.at[:, i * width : (i + 1) * width],
            ds_hbm.at[tiles * heads + i],
            sems_out.at[2, i, 1],
        )
        for i in range(2)
    ]
    stats_fetch = pltpu.make_async_copy(
        stats_hbm.at[:, :, 0 : stats.shape[2]], stats, sems_in.at[0, heads]
    )
    for copy in fetches(0):
        copy.start()
    stats_fetch.start()
    for copy in kv_stores:
        copy.start()

    query_mask[...] = mask_of_queries(rows)
    shape = (trunk, HEAD_SIZE)
    column, row = iota(shape, 1), iota(shape, 0)
    for t in range(tiles):
        key_mask[t] = jnp.where(
            (column == rows) & (row > parents[tree, t]), MASKED, 0.0
        ).astype(jnp.bfloat16)
    lane_row = jnp.bitwise_and(iota((1, CHUNK), 1), rows - 1)
    live = [jnp.where(lane_row < lengths[tree, t], 1.0, 0.0) for t in range(tiles)]

    stats_fetch.wait()

    def matmuls(h, t, half):
        tile = slice(t * rows, (t + 1) * rows)
        queries = stacked(q, h, tile, half * per_chunk, per_chunk)
        grads = stacked(do, h, tile, half * per_chunk, per_chunk)
        scores = dot_nt(
            jnp.concatenate([kv[:, lanes(h * HEAD_SIZE)], key_mask[t]], axis=1),
            jnp.concatenate([queries, query_mask[...]], axis=1),
        )
        return scores, dot_nt(kv[:, lanes(width + h * HEAD_SIZE)], grads)

    def softmax(h, t, half, score, grad):
        part = slice(half * CHUNK, (half + 1) * CHUNK)
        branch_peak = stats[t, h, 0:1, part]
        peak = jnp.maximum(jnp.max(score, axis=0, keepdims=True), branch_peak)
        e = jnp.exp2((score - peak) * to_exp2)
        shrink = jnp.exp2((branch_peak - peak) * to_exp2)
        inv = live[t] / (jnp.sum(e, axis=0, keepdims=True) + shrink * stats[t, h, 1:2, part])
        delta = inv * (
            jnp.sum(e * grad, axis=0, keepdims=True) + shrink * stats[t, h, 2:3, part]
        )
        weights = e * inv
        ds_buf[t, h, :, part] = (weights * (grad - delta)).astype(jnp.bfloat16)
        low_buf[t, :, part] = weights.astype(jnp.bfloat16)
        row_buf[t, h, 0:1, part] = shrink * inv
        row_buf[t, h, 1:2, part] = delta
        row_buf[t, h, 2:, part] = jnp.zeros((row_buf.shape[2] - 2, CHUNK), jnp.float32)

    def trunk_parts(h, t):
        count = per_chunk * halves
        tile = slice(t * rows, (t + 1) * rows)
        left = jnp.concatenate([ds_buf[t, h], low_buf[t]], axis=0)
        right = jnp.concatenate(
            [stacked(q, h, tile, 0, count), stacked(do, h, tile, 0, count)], axis=1
        )
        both = dot_nn(left, right)
        return both[:trunk, :HEAD_SIZE], both[trunk:, HEAD_SIZE:]

    order = [(t, half) for t in range(tiles) for half in range(halves)]

    def head_step(h, carry):
        totals = None
        for copy in fetches(h):
            copy.wait()

        @pl.when(h + 1 < heads)
        def _():
            for copy in fetches(h + 1):
                copy.start()

        ahead = matmuls(h, *order[0])
        for c, (t, half) in enumerate(order):
            now = ahead
            if c + 1 < len(order):
                ahead = matmuls(h, *order[c + 1])
            softmax(h, t, half, *now)
            if half == halves - 1:
                for copy in tile_stores(h, t):
                    copy.start()
                parts = trunk_parts(h, t)
                totals = parts if t == 0 else tuple(a + b for a, b in zip(totals, parts))
        shape = (sums.shape[1], sums.shape[3], HEAD_SIZE)
        sums[h, :, 0] = (totals[0] * scale).reshape(shape).astype(jnp.bfloat16)
        sums[h, :, 1] = totals[1].reshape(shape).astype(jnp.bfloat16)
        sum_store(h).start()
        return carry

    lax.fori_loop(0, heads, head_step, 0)
    for copy in kv_stores:
        copy.wait()
    for h in range(heads):
        sum_store(h).wait()
        for t in range(tiles):
            for copy in tile_stores(h, t):
                copy.wait()


def grad_kernel(
    q_hbm,
    do_hbm,
    kb_hbm,
    ds_hbm,
    e_hbm,
    g_hbm,
    rows_hbm,
    dq,
    dkb,
    dvb,
    q,
    do,
    kv,
    kb,
    ds,
    e,
    g,
    row_values,
    dq_buf,
    dkb_buf,
    dvb_buf,
    sems_in,
    sems,
    *,
    tiles,
):
    rows = q_hbm.shape[0] // tiles
    width = kb_hbm.shape[1]
    heads = width // HEAD_SIZE
    group_width = q_hbm.shape[1] // heads
    groups = group_width // HEAD_SIZE
    scale = 1.0 / math.sqrt(HEAD_SIZE)

    def fetches(t):
        tile = pl.ds(pl.multiple_of(t * rows, rows), rows)
        return [
            pltpu.make_async_copy(source.at[part], buf.at[part], sems_in.at[i, t])
            for i, (source, buf, part) in enumerate(
                (
                    (q_hbm, q, tile),
                    (do_hbm, do, tile),
                    (e_hbm, e, t),
                    (g_hbm, g, t),
                    (kb_hbm, kb, tile),
                )
            )
        ]

    kv_fetches = [
        pltpu.make_async_copy(
            ds_hbm.at[tiles * heads + i],
            kv.at[:, i * width : (i + 1) * width],
            sems_in.at[7, i],
        )
        for i in range(2)
    ]
    for copy in kv_fetches:
        copy.start()
    def computed_fetches(t):
        return [
            pltpu.make_async_copy(
                ds_hbm.at[pl.ds(pl.multiple_of(t * heads, heads), heads)],
                ds.at[t],
                sems_in.at[5, t],
            ),
            pltpu.make_async_copy(
                rows_hbm.at[t, :, 0 : row_values.shape[2]], row_values.at[t], sems_in.at[6, t]
            ),
        ]

    for t in range(tiles):
        for copy in fetches(t) + computed_fetches(t):
            copy.start()
    for copy in kv_fetches:
        copy.wait()

    def copies(t):
        tile = pl.ds(pl.multiple_of(t * rows, rows), rows)
        return [
            pltpu.make_async_copy(buf.at[tile], out.at[tile], sems.at[i, t])
            for i, (buf, out) in enumerate(((dq_buf, dq), (dkb_buf, dkb), (dvb_buf, dvb)))
        ]

    def tile_step(t, carry):
        for copy in fetches(t) + computed_fetches(t):
            copy.wait()
        tile = pl.ds(pl.multiple_of(t * rows, rows), rows)

        def all_heads(ref, h):
            return jnp.concatenate(
                [ref[tile, lanes(h * group_width + j * HEAD_SIZE)] for j in range(groups)], axis=0
            )

        for h in range(heads):
            span = lanes(h * HEAD_SIZE)
            keys = jnp.concatenate([kv[:, span], kb[tile, span]], axis=0)
            weights = e[t, h].astype(jnp.float32) * row_values[t, h, 0:1, :]
            branch_ds = weights * (g[t, h].astype(jnp.float32) - row_values[t, h, 1:2, :])
            branch_ds = branch_ds.astype(jnp.bfloat16)
            dkb_buf[tile, span] = dot_nn(branch_ds, all_heads(q, h)) * scale
            dvb_buf[tile, span] = dot_nn(weights.astype(jnp.bfloat16), all_heads(do, h))
            got = (dot_tn(keys, jnp.concatenate([ds[t, h], branch_ds], axis=0)) * scale).T
            for j in range(groups):
                dq_buf[tile, lanes(h * group_width + j * HEAD_SIZE)] = got[
                    j * rows : (j + 1) * rows
                ]
        for copy in copies(t):
            copy.start()
        return carry

    lax.fori_loop(0, tiles, tile_step, 0)
    for t in range(tiles):
        for copy in copies(t):
            copy.wait()


def per_device(
    queries,
    branch_key_rows,
    branch_value_rows,
    grad_output,
    trunk_keys,
    trunk_token_values,
    lengths,
    parents,
):
    q = queries[0]
    do = grad_output[0]
    kb = branch_key_rows[0]
    vb = branch_value_rows[0]
    seq = lax.axis_size("seq")
    leaf = lax.axis_index("leaf").astype(jnp.int32).reshape(1)
    tiles = lengths.shape[1]
    rows = q.shape[0] // tiles
    width = kb.shape[1]
    heads = width // HEAD_SIZE
    wide = q.shape[1] // width * rows
    own = trunk_keys.shape[1]
    trunk = own * seq
    work = heads * tiles * wide * (trunk + rows) * HEAD_SIZE * 2

    both = jnp.concatenate([trunk_keys[0], trunk_token_values[0]], axis=1)
    spread = jnp.broadcast_to(both[None], (seq,) + both.shape)
    gathered = lax.all_to_all(spread, "seq", 0, 0, tiled=True).reshape(trunk, 2 * width)

    vmem = pl.BlockSpec(memory_space=pltpu.VMEM)
    smem = pl.BlockSpec(memory_space=pltpu.SMEM)
    hbm = pl.BlockSpec(memory_space=pltpu.HBM)
    ds_shape = (tiles, heads, trunk, wide)
    branch_shape = (tiles, heads, rows, wide)
    stats_shape = (tiles, heads, 8, wide)
    kept_shape = (tiles, heads, rows + 16, wide)
    head_shape = (heads, tiles * rows, q.shape[1] // heads)

    e, g, stats = pl.pallas_call(
        lambda *refs: local_kernel(*refs, tiles=tiles),
        in_specs=[hbm] * 4,
        out_specs=[hbm] * 3,
        out_shape=[
            jax.ShapeDtypeStruct(branch_shape, jnp.bfloat16),
            jax.ShapeDtypeStruct(branch_shape, jnp.bfloat16),
            jax.ShapeDtypeStruct(kept_shape, jnp.float32),
        ],
        scratch_shapes=[
            pltpu.VMEM(head_shape, jnp.bfloat16),
            pltpu.VMEM(head_shape, jnp.bfloat16),
            pltpu.VMEM(kb.shape, jnp.bfloat16),
            pltpu.VMEM(vb.shape, jnp.bfloat16),
            pltpu.VMEM(branch_shape, jnp.bfloat16),
            pltpu.VMEM(branch_shape, jnp.bfloat16),
            pltpu.VMEM(stats_shape, jnp.float32),
            pltpu.VMEM((CHUNK, HEAD_SIZE), jnp.bfloat16),
            pltpu.SemaphoreType.DMA((2, heads + 1)),
            pltpu.SemaphoreType.DMA((3, heads)),
        ],
        compiler_params=pltpu.CompilerParams(vmem_limit_bytes=65_900_000),
        cost_estimate=pl.CostEstimate(flops=2 * work, bytes_accessed=7 << 20, transcendentals=0),
        name="local",
    )(q, do, kb, vb)

    sums, ds, row_values = pl.pallas_call(
        lambda *refs: score_kernel(*refs, tiles=tiles),
        in_specs=[smem] * 3 + [hbm, hbm, vmem, hbm],
        out_specs=[hbm] * 3,
        out_shape=[
            jax.ShapeDtypeStruct((seq, 2, own, width), jnp.bfloat16),
            jax.ShapeDtypeStruct((tiles * heads + 2, trunk, wide), jnp.bfloat16),
            jax.ShapeDtypeStruct(kept_shape, jnp.float32),
        ],
        scratch_shapes=[
            pltpu.VMEM(head_shape, jnp.bfloat16),
            pltpu.VMEM(head_shape, jnp.bfloat16),
            pltpu.VMEM(stats_shape, jnp.float32),
            pltpu.VMEM((heads, seq, 2, own, HEAD_SIZE), jnp.bfloat16),
            pltpu.VMEM(ds_shape, jnp.bfloat16),
            pltpu.VMEM(stats_shape, jnp.float32),
            pltpu.VMEM((tiles, trunk, wide), jnp.bfloat16),
            pltpu.VMEM((tiles, trunk, HEAD_SIZE), jnp.bfloat16),
            pltpu.VMEM((CHUNK, HEAD_SIZE), jnp.bfloat16),
            pltpu.SemaphoreType.DMA((2, heads + 1)),
            pltpu.SemaphoreType.DMA((3, heads, tiles)),
        ],
        compiler_params=pltpu.CompilerParams(vmem_limit_bytes=53_500_000),
        cost_estimate=pl.CostEstimate(
            flops=4 * work, bytes_accessed=12 << 20, transcendentals=work // 256
        ),
        name="scores",
    )(leaf, lengths, parents, q, do, gathered, stats)

    shares = lax.all_to_all(sums, "seq", 0, 0, tiled=True)

    dq, dkb, dvb = pl.pallas_call(
        lambda *refs: grad_kernel(*refs, tiles=tiles),
        in_specs=[hbm] * 7,
        out_specs=[hbm] * 3,
        out_shape=[
            jax.ShapeDtypeStruct(q.shape, jnp.float32),
            jax.ShapeDtypeStruct(kb.shape, jnp.float32),
            jax.ShapeDtypeStruct(vb.shape, jnp.float32),
        ],
        scratch_shapes=[
            pltpu.VMEM(q.shape, jnp.bfloat16),
            pltpu.VMEM(q.shape, jnp.bfloat16),
            pltpu.VMEM(gathered.shape, jnp.bfloat16),
            pltpu.VMEM(kb.shape, jnp.bfloat16),
            pltpu.VMEM(ds_shape, jnp.bfloat16),
            pltpu.VMEM(branch_shape, jnp.bfloat16),
            pltpu.VMEM(branch_shape, jnp.bfloat16),
            pltpu.VMEM(stats_shape, jnp.float32),
            pltpu.VMEM(q.shape, jnp.float32),
            pltpu.VMEM(kb.shape, jnp.float32),
            pltpu.VMEM(vb.shape, jnp.float32),
            pltpu.SemaphoreType.DMA((8, tiles)),
            pltpu.SemaphoreType.DMA((3, tiles)),
        ],
        compiler_params=pltpu.CompilerParams(vmem_limit_bytes=65_900_000),
        cost_estimate=pl.CostEstimate(flops=2 * work, bytes_accessed=16 << 20, transcendentals=0),
        name="grads",
    )(q, do, kb, ds, e, g, row_values)

    trunk_grads = jnp.sum(shares.astype(jnp.float32), axis=0)
    return dq[None], dkb[None], dvb[None], trunk_grads[0][None], trunk_grads[1][None]


def solution(mesh):
    split = P("leaf", "seq", None)
    return jax.shard_map(
        per_device,
        mesh=mesh,
        in_specs=(split,) * 6 + (P(None, "seq"),) * 2,
        out_specs=(split,) * 5,
        check_vma=False,
    )
```
